32 devices in a mesh: grp: 2 (over y), blk: 8 (over z, x), uly: 2 (over core).
Axes of the slice: x: 2, y: 2, z: 4, core: 2. Of those that a mesh axis runs over, the one named last changes fastest.
Arguments:
- query: bfloat16 [512, 1152], P(('grp', 'blk', 'uly')), parts along dimension 0, may hold values from -6 to 6
- key: bfloat16 [512, 1152], P(('grp', 'blk', 'uly')), parts along dimension 0, may hold values from -6 to 6
- value: bfloat16 [512, 1152], P(('grp', 'blk', 'uly')), parts along dimension 0, may hold values from -6 to 6
- q_gain: float32 [96], replicated, may hold values from 1 to 2.5
- k_gain: float32 [96], replicated, may hold values from 1 to 2.5
- out_weight: bfloat16 [1152, 2304], P('uly'), may hold values from -0.1875 to 0.1875
Outputs:
- mixed: bfloat16 [512, 2304], P(('grp', 'blk', 'uly')), parts along dimension 0
The draws below stay inside these ranges and needn't reach their ends.
There are 2 independent parts, one for each index of `grp`. The reference program is written for one: setup_inputs(seed, part) draws one part's arguments, and reference() takes and returns one part's arrays. A program takes and returns all parts, laid end to end along the dimension named above; an argument that names none is the same for every part. Nothing has to cross between parts.
All inputs are finite; a program needn't handle non-finite values.
Results may differ from the reference program's by a relative error of at most 0.012.
Values may be sent and summed in bfloat16 or wider, within the bound.
A program may use at most 128 MiB of HBM per device.

```python
import jax
import jax.numpy as jnp
from jax import lax

H = 12
HD = 96
D = 2304
S = 256


def steps_of(stream_key, extent, pieces, least, top_value):
    def one(position, shards_of):
        heights = jax.random.uniform(jax.random.fold_in(jax.random.fold_in(stream_key, 6), position), (shards_of,), jnp.float32, least / len(pieces), top_value / len(pieces))
        return jnp.repeat(jnp.exp(heights), extent[position] // shards_of).reshape((-1,) + (1,) * (len(extent) - position - 1))

    level = one(*pieces[0])
    for cut in pieces[1:]:
        level = level * one(*cut)
    return level


def normal_values(rng, shape, spread, most, shards=(), dtype=jnp.bfloat16):
    loudness = steps_of(rng, shape, shards, -0.22, 0.18) if shards else 1.0
    drawn = jax.random.normal(rng, shape, jnp.float32) * spread * loudness
    return jnp.minimum(jnp.maximum(drawn, -most), most).astype(dtype)


def setup_inputs(seed: int = 0, part: int = 0) -> dict:
    seeds = jax.random.split(jax.random.key(seed), 7)
    part_splits = jax.random.split(jax.random.fold_in(seeds[6], part), 7)
    query = normal_values(part_splits[0], (S, H * HD), 1.0, 6.0, ((0, 16),))
    key = normal_values(part_splits[1], (S, H * HD), 1.0, 6.0, ((0, 16),))
    value = normal_values(part_splits[2], (S, H * HD), 1.0, 6.0, ((0, 16),))
    q_gain = jnp.clip(jax.random.uniform(seeds[3], (HD,), jnp.float32, 1.0, 2.5), 1.0, 2.5)
    k_gain = jnp.clip(jax.random.uniform(seeds[4], (HD,), jnp.float32, 1.0, 2.5), 1.0, 2.5)
    out_weight = normal_values(seeds[5], (H * HD, D), (H * HD) ** -0.5, 0.1875, ((0, 2),))
    return {"query": query, "key": key, "value": value, "q_gain": q_gain, "k_gain": k_gain, "out_weight": out_weight}


def normed(data, gain):
    count = data.shape[0]
    grid = data.astype(jnp.float32).reshape(count, H, HD)
    meansq = lax.optimization_barrier(jnp.mean(grid * grid, axis=-1, keepdims=True))
    return (grid * lax.rsqrt(meansq + 1e-06) * gain).astype(jnp.bfloat16)

def reference(query, key, value, q_gain, k_gain, out_weight):
    count = query.shape[0]
    query_heads = jnp.transpose(normed(query, q_gain), (1, 0, 2))
    key_heads = jnp.transpose(normed(key, k_gain), (1, 0, 2))
    value_heads = jnp.transpose(value.reshape(count, H, HD), (1, 0, 2))
    score_scale = float(HD) ** (-0.5)

    def one_head(operands):
        query_one, key_one, value_one = operands
        scores = jnp.dot(query_one, key_one.T, preferred_element_type=jnp.float32) * score_scale
        expd = jnp.exp(scores)
        total_weight = lax.optimization_barrier(jnp.sum(expd, axis=1))
        weighted = jnp.dot(expd.astype(jnp.bfloat16), value_one, preferred_element_type=jnp.float32)
        return (weighted / total_weight[:, None]).astype(jnp.bfloat16)
    attn = lax.map(one_head, (query_heads, key_heads, value_heads))
    attn = jnp.transpose(attn, (1, 0, 2)).reshape(count, H * HD)
    return jnp.dot(attn, out_weight, preferred_element_type=jnp.float32).astype(jnp.bfloat16)
```

```python
import functools

import jax
import jax.numpy as jnp
from jax import lax
from jax.experimental import pallas as pl
from jax.experimental.pallas import tpu as pltpu
from jax.sharding import PartitionSpec as P

HD = 96
LANES = 128
MESH = pl.DeviceIdType.MESH


def loop(count, body):
    if count <= 32:
        for i in range(count):
            body(i)
    else:
        lax.fori_loop(0, count, lambda i, c: (body(i), c)[1], 0)


def layer_kernel(
    blks, ulys, heads, copies,
    q_hbm, k_hbm, v_hbm, qg_ref, kg_ref, w_hbm, out_ref,
    raw, w_vmem, pack, qkv, attn, back, mine, away, arrived,
    load_sem, w_sem, send1, recv1, send2, recv2, send3, recv3,
):
    n = blks * ulys
    rows = raw.shape[1]
    owners = heads * copies
    blk, uly = lax.axis_index("blk"), lax.axis_index("uly")
    me = blk * ulys + uly
    chip_rows = rows * ulys
    core_heads = heads // ulys
    seq = n * rows
    block = seq // copies
    chips = block // chip_rows

    loads = [
        pltpu.make_async_copy(src, raw.at[i], load_sem.at[i])
        for i, src in enumerate((q_hbm, k_hbm, v_hbm))
    ]
    for one in loads:
        one.start()
    load_w = pltpu.make_async_copy(w_hbm, w_vmem, w_sem)
    load_w.start()

    def mirror(d):
        plane = d // 4
        return d + (plane % 2) * (3 - 2 * (d % 4))

    def owner_device(o):
        return mirror(o * n // owners)

    spot = mirror(me)
    slot = (spot * owners + n - 1) // n
    is_owner = jnp.logical_and(slot < owners, (slot * n) // owners == spot)
    slot = jnp.minimum(slot, owners - 1)

    barrier = pltpu.get_barrier_semaphore()

    def greet(i):
        d = lax.rem(me + 1 + i, n)
        pl.semaphore_signal(
            barrier, inc=1, device_id={"blk": d // ulys, "uly": d % ulys}, device_id_type=MESH
        )

    loop(n - 1, greet)

    pad = jnp.zeros((rows, LANES - HD), jnp.bfloat16)
    for i, gain_ref in ((0, qg_ref), (1, kg_ref)):
        loads[i].wait()
        gain = gain_ref[...]
        for h in range(heads):
            x = raw[i, :, h * HD:(h + 1) * HD].astype(jnp.float32)
            scale = lax.rsqrt(jnp.mean(x * x, axis=-1, keepdims=True) + 1e-06)
            normed = (x * scale * gain).astype(jnp.bfloat16)
            pack[h, :, i * LANES:(i + 1) * LANES] = jnp.concatenate([normed, pad], axis=1)
    loads[2].wait()
    for h in range(heads):
        x = raw[2, :, h * HD:(h + 1) * HD]
        pack[h, :, 2 * LANES:3 * LANES] = jnp.concatenate([x, pad], axis=1)

    pl.semaphore_wait(barrier, n - 1)

    my_rows = pl.ds(pl.multiple_of(me * rows, rows), rows)

    def send_of(o):
        d = owner_device(o)
        return d, pltpu.make_async_remote_copy(
            src_ref=pack.at[o // copies],
            dst_ref=qkv.at[my_rows],
            send_sem=send1.at[o],
            recv_sem=recv1.at[me],
            device_id={"blk": d // ulys, "uly": d % ulys},
            device_id_type=MESH,
        )

    start_at = (me * owners) // n + owners // 2

    def send(i):
        d, copy = send_of(lax.rem(start_at + i, owners))

        @pl.when(d != me)
        def _():
            copy.start()

    loop(owners, send)

    @pl.when(is_owner)
    def _():
        head = slot // copies
        part = slot % copies
        qkv[my_rows, :] = pack[head]

        def got(i):
            d = lax.rem(me + 1 + i, n)
            pltpu.make_async_remote_copy(
                src_ref=pack.at[0],
                dst_ref=qkv.at[pl.ds(pl.multiple_of(d * rows, rows), rows)],
                send_sem=send1.at[0],
                recv_sem=recv1.at[d],
                device_id={"blk": blk, "uly": uly},
                device_id_type=MESH,
            ).wait_recv()

        loop(n - 1, got)
        query = qkv[pl.ds(pl.multiple_of(part * block, block), block), 0:LANES]
        score_scale = float(HD) ** (-0.5)

        def step(j, carry):
            weighted, total = carry
            here = pl.ds(j * block, block)
            keys = qkv[here, LANES:2 * LANES]
            values = qkv[here, 2 * LANES:3 * LANES]
            scores = lax.dot_general(
                query, keys, (((1,), (1,)), ((), ())), preferred_element_type=jnp.float32
            ) * score_scale
            expd = jnp.exp(scores)
            total = total + jnp.sum(expd, axis=-1, keepdims=True)
            weighted = weighted + jnp.dot(
                expd.astype(jnp.bfloat16), values, preferred_element_type=jnp.float32
            )
            return weighted, total

        carry = (jnp.zeros((block, LANES), jnp.float32), jnp.zeros((block, 1), jnp.float32))
        if copies == 1:
            weighted, total = step(0, carry)
        else:
            weighted, total = lax.fori_loop(
                0, copies, lambda j, c: step(pl.multiple_of(j, 1), c), carry
            )
        attn[...] = (weighted / total).astype(jnp.bfloat16)

        to_core = head // core_heads
        place = head % core_heads

        def result_copy(i):
            chip = part * chips + i
            return chip, pltpu.make_async_remote_copy(
                src_ref=attn.at[pl.ds(i * chip_rows, chip_rows)],
                dst_ref=back.at[place],
                send_sem=send2.at[i],
                recv_sem=recv2.at[place],
                device_id={"blk": chip, "uly": to_core},
                device_id_type=MESH,
            )

        def local_copy(i):
            return pltpu.make_async_copy(
                attn.at[pl.ds(i * chip_rows, chip_rows)], back.at[place], recv2.at[place]
            )

        def give(i):
            chip, copy = result_copy(i)
            home = chip * ulys + to_core == me

            @pl.when(home)
            def _():
                local_copy(i).start()

            @pl.when(jnp.logical_not(home))
            def _():
                copy.start()

        loop(chips, give)

        def given(i):
            chip, copy = result_copy(i)

            @pl.when(chip * ulys + to_core != me)
            def _():
                copy.wait_send()

        loop(chips, given)

    for h in range(core_heads):
        pltpu.make_async_copy(attn.at[pl.ds(0, chip_rows)], back.at[h], recv2.at[h]).wait()

    own_rows = pl.ds(pl.multiple_of(uly * rows, rows), rows)
    other_rows = pl.ds(pl.multiple_of((1 - uly) * rows, rows), rows)
    lhs = jnp.concatenate(
        [
            jnp.concatenate([back[h, other_rows, 0:HD] for h in range(core_heads)], axis=1),
            jnp.concatenate([back[h, own_rows, 0:HD] for h in range(core_heads)], axis=1),
        ],
        axis=0,
    )
    load_w.wait()
    pieces = send3.shape[0]
    width = out_ref.shape[1] // pieces
    swaps = []
    for c in range(pieces):
        cols = slice(c * width, (c + 1) * width)
        part_out = jnp.dot(lhs, w_vmem[:, cols], preferred_element_type=jnp.float32)
        away[c] = part_out[:rows]
        mine[c] = part_out[rows:]
        swap = pltpu.make_async_remote_copy(
            src_ref=away.at[c],
            dst_ref=arrived.at[c],
            send_sem=send3.at[c],
            recv_sem=recv3.at[c],
            device_id={"blk": blk, "uly": 1 - uly},
            device_id_type=MESH,
        )
        swap.start()
        swaps.append(swap)
    for c in range(pieces):
        swaps[c].wait_recv()
        out_ref[:, c * width:(c + 1) * width] = (mine[c] + arrived[c]).astype(out_ref.dtype)

    for swap in swaps:
        swap.wait_send()

    def sent(o):
        d, copy = send_of(o)

        @pl.when(d != me)
        def _():
            copy.wait_send()

    loop(owners, sent)


def on_device(blks, ulys, query, key, value, q_gain, k_gain, out_weight):
    rows, width = query.shape
    heads = width // HD
    n = blks * ulys
    copies = 1
    while heads * copies * 2 <= n:
        copies *= 2
    owners = heads * copies
    depth, cols = out_weight.shape
    seq = n * rows
    block = seq // copies
    chip_rows = rows * ulys
    pieces = 3
    dma = pltpu.SemaphoreType.DMA
    return pl.pallas_call(
        functools.partial(layer_kernel, blks, ulys, heads, copies),
        out_shape=jax.ShapeDtypeStruct((rows, cols), jnp.bfloat16),
        in_specs=[
            pl.BlockSpec(memory_space=pl.ANY),
            pl.BlockSpec(memory_space=pl.ANY),
            pl.BlockSpec(memory_space=pl.ANY),
            pl.BlockSpec(memory_space=pltpu.VMEM),
            pl.BlockSpec(memory_space=pltpu.VMEM),
            pl.BlockSpec(memory_space=pl.ANY),
        ],
        out_specs=pl.BlockSpec(memory_space=pltpu.VMEM),
        scratch_shapes=[
            pltpu.VMEM((3, rows, width), jnp.bfloat16),
            pltpu.VMEM((depth, cols), jnp.bfloat16),
            pltpu.VMEM((heads, rows, 3 * LANES), jnp.bfloat16),
            pltpu.VMEM((seq, 3 * LANES), jnp.bfloat16),
            pltpu.VMEM((block, LANES), jnp.bfloat16),
            pltpu.VMEM((heads // ulys, chip_rows, LANES), jnp.bfloat16),
            pltpu.VMEM((pieces, rows, cols // pieces), jnp.float32),
            pltpu.VMEM((pieces, rows, cols // pieces), jnp.float32),
            pltpu.VMEM((pieces, rows, cols // pieces), jnp.float32),
            dma((3,)),
            dma,
            dma((owners,)),
            dma((n,)),
            dma((block // chip_rows,)),
            dma((heads // ulys,)),
            dma((pieces,)),
            dma((pieces,)),
        ],
        compiler_params=pltpu.CompilerParams(collective_id=0, has_side_effects=True),
    )(query, key, value, q_gain.reshape(1, HD), k_gain.reshape(1, HD), out_weight)


def solution(mesh):
    blks, ulys = mesh.shape["blk"], mesh.shape["uly"]
    tokens = P(("grp", "blk", "uly"), None)
    return jax.shard_map(
        functools.partial(on_device, blks, ulys),
        mesh=mesh,
        in_specs=(tokens, tokens, tokens, P(), P(), P("uly", None)),
        out_specs=tokens,
        check_vma=False,
    )
```

```python
import functools

import jax
import jax.numpy as jnp
from jax import lax
from jax.experimental import pallas as pl
from jax.experimental.pallas import tpu as pltpu
from jax.sharding import PartitionSpec as P

HD = 96
LANES = 128
CHUNKS = 4
MESH = pl.DeviceIdType.MESH


def loop(count, body):
    if count <= 32:
        for i in range(count):
            body(i)
    else:
        lax.fori_loop(0, count, lambda i, c: (body(i), c)[1], 0)


def layer_kernel(
    blks, ulys, heads, copies,
    q_hbm, k_hbm, v_hbm, qg_hbm, kg_hbm, w_hbm, out_ref,
    raw, gains, w_vmem, pack, qkv, attn, back, acc,
    load_sem, gain_sem, w_sem, send1, recv1, send2, recv2, send_w, recv_w,
):
    n = blks * ulys
    rows = raw.shape[1]
    owners = heads * copies
    blk, uly = lax.axis_index("blk"), lax.axis_index("uly")
    me = blk * ulys + uly
    seq = n * rows
    block = seq // copies
    chunk = attn.shape[1]
    chunks = attn.shape[0]
    targets = chunk // rows
    depth = w_hbm.shape[0]
    upper = (2 * me) // n

    loads = [
        pltpu.make_async_copy(src, raw.at[i], load_sem.at[i])
        for i, src in enumerate((q_hbm, k_hbm, v_hbm))
    ]
    load_gains = [
        pltpu.make_async_copy(src, gains.at[i], gain_sem.at[i])
        for i, src in enumerate((qg_hbm, kg_hbm))
    ]
    for one in loads + load_gains:
        one.start()

    def mirror(d):
        plane = d // 4
        return d + (plane % 2) * (3 - 2 * (d % 4))

    def owner_device(o):
        return mirror(o * n // owners)

    spot = mirror(me)
    slot = (spot * owners + n - 1) // n
    is_owner = jnp.logical_and(slot < owners, (slot * n) // owners == spot)
    slot = jnp.minimum(slot, owners - 1)

    barrier = pltpu.get_barrier_semaphore()

    def greet(i):
        d = lax.rem(me + 1 + i, n)
        pl.semaphore_signal(
            barrier, inc=1, device_id={"blk": d // ulys, "uly": d % ulys}, device_id_type=MESH
        )

    loop(n - 1, greet)

    my_depth = pl.ds(pl.multiple_of(uly * depth, depth), depth)
    load_w = pltpu.make_async_copy(w_hbm, w_vmem.at[my_depth], w_sem)
    load_w.start()

    pad = jnp.zeros((rows, LANES - HD), jnp.bfloat16)
    for i in range(2):
        loads[i].wait()
        load_gains[i].wait()
        gain = gains[i]
        for h in range(heads):
            x = raw[i, :, h * HD:(h + 1) * HD].astype(jnp.float32)
            scale = lax.rsqrt(jnp.mean(x * x, axis=-1, keepdims=True) + 1e-06)
            normed = (x * scale * gain).astype(jnp.bfloat16)
            pack[h, :, i * LANES:(i + 1) * LANES] = jnp.concatenate([normed, pad], axis=1)
    loads[2].wait()
    for h in range(heads):
        x = raw[2, :, h * HD:(h + 1) * HD]
        pack[h, :, 2 * LANES:3 * LANES] = jnp.concatenate([x, pad], axis=1)

    pl.semaphore_wait(barrier, n - 1)

    my_rows = pl.ds(pl.multiple_of(me * rows, rows), rows)

    def send_of(o):
        d = owner_device(o)
        return d, pltpu.make_async_remote_copy(
            src_ref=pack.at[o // copies],
            dst_ref=qkv.at[my_rows],
            send_sem=send1.at[o],
            recv_sem=recv1.at[me],
            device_id={"blk": d // ulys, "uly": d % ulys},
            device_id_type=MESH,
        )

    start_at = (me * owners) // n + owners // 2

    def send(i):
        d, copy = send_of(lax.rem(start_at + i, owners))

        @pl.when(d != me)
        def _():
            copy.start()

    loop(owners, send)

    give_w = pltpu.make_async_remote_copy(
        src_ref=w_hbm,
        dst_ref=w_vmem.at[my_depth],
        send_sem=send_w,
        recv_sem=recv_w,
        device_id={"blk": blk, "uly": 1 - uly},
        device_id_type=MESH,
    )
    give_w.start()

    @pl.when(is_owner)
    def _():
        head = slot // copies
        part = slot % copies
        qkv[my_rows, :] = pack[head]

        def got(i):
            d = lax.rem(me + 1 + i, n)
            pltpu.make_async_remote_copy(
                src_ref=pack.at[0],
                dst_ref=qkv.at[pl.ds(pl.multiple_of(d * rows, rows), rows)],
                send_sem=send1.at[0],
                recv_sem=recv1.at[d],
                device_id={"blk": blk, "uly": uly},
                device_id_type=MESH,
            ).wait_recv()

        loop(n - 1, got)
        score_scale = float(HD) ** (-0.5)

        def step(query, j, carry):
            weighted, total = carry
            here = pl.ds(j * block, block)
            keys = qkv[here, LANES:2 * LANES]
            values = qkv[here, 2 * LANES:3 * LANES]
            scores = lax.dot_general(
                query, keys, (((1,), (1,)), ((), ())), preferred_element_type=jnp.float32
            ) * score_scale
            expd = jnp.exp(scores)
            total = total + jnp.sum(expd, axis=-1, keepdims=True)
            weighted = weighted + jnp.dot(
                expd.astype(jnp.bfloat16), values, preferred_element_type=jnp.float32
            )
            return weighted, total

        def result_copies(c):
            for i in range(targets):
                d = (part * chunks + c) * targets + i
                src = attn.at[c, pl.ds(i * rows, rows)]
                yield (
                    d == me,
                    functools.partial(
                        pltpu.make_async_copy, src, back.at[head], recv2.at[head]
                    ),
                    pltpu.make_async_remote_copy(
                        src_ref=src,
                        dst_ref=back.at[head],
                        send_sem=send2.at[c * targets + i],
                        recv_sem=recv2.at[head],
                        device_id={"blk": d // ulys, "uly": d % ulys},
                        device_id_type=MESH,
                    ),
                )

        for k in range(chunks):
            c = chunks - 1 - k + upper * (2 * k + 1 - chunks)
            at = part * block + c * chunk
            query = qkv[pl.ds(pl.multiple_of(at, chunk), chunk), 0:LANES]
            carry = (jnp.zeros((chunk, LANES), jnp.float32), jnp.zeros((chunk, 1), jnp.float32))
            if copies == 1:
                weighted, total = step(query, 0, carry)
            else:
                weighted, total = lax.fori_loop(
                    0, copies, functools.partial(lambda q, j, c: step(q, j, c), query), carry
                )
            attn[c] = (weighted / total).astype(jnp.bfloat16)
            for home, local, remote in result_copies(c):
                pl.when(home)(lambda local=local: local().start())
                pl.when(jnp.logical_not(home))(remote.start)

        for c in range(chunks):
            for home, _, remote in result_copies(c):
                pl.when(jnp.logical_not(home))(remote.wait_send)

    load_w.wait()
    give_w.wait_recv()
    first = (me * heads) // n
    for i in range(heads):
        h = lax.rem(first + i * (1 - 2 * upper) + heads, heads)
        pltpu.make_async_copy(attn.at[0, pl.ds(0, rows)], back.at[h], recv2.at[h]).wait()
        term = jnp.dot(
            back[h, :, 0:HD],
            w_vmem[pl.ds(pl.multiple_of(h * HD, HD), HD), :],
            preferred_element_type=jnp.float32,
        )
        if i == 0:
            acc[...] = term
        elif i < heads - 1:
            acc[...] += term
        else:
            out_ref[...] = (acc[...] + term).astype(out_ref.dtype)

    give_w.wait_send()

    def sent(o):
        d, copy = send_of(o)

        @pl.when(d != me)
        def _():
            copy.wait_send()

    loop(owners, sent)


def on_device(blks, ulys, query, key, value, q_gain, k_gain, out_weight):
    rows, width = query.shape
    heads = width // HD
    n = blks * ulys
    copies = 1
    while heads * copies * 2 <= n:
        copies *= 2
    owners = heads * copies
    depth, cols = out_weight.shape
    seq = n * rows
    block = seq // copies
    chunks = CHUNKS
    dma = pltpu.SemaphoreType.DMA
    return pl.pallas_call(
        functools.partial(layer_kernel, blks, ulys, heads, copies),
        out_shape=pltpu.VMEM((rows, cols), jnp.bfloat16),
        in_specs=[pl.BlockSpec(memory_space=pltpu.HBM)] * 6,
        out_specs=pl.BlockSpec(memory_space=pltpu.VMEM),
        scratch_shapes=[
            pltpu.VMEM((3, rows, width), jnp.bfloat16),
            pltpu.VMEM((2, 1, HD), jnp.float32),
            pltpu.VMEM((width, cols), jnp.bfloat16),
            pltpu.VMEM((heads, rows, 3 * LANES), jnp.bfloat16),
            pltpu.VMEM((seq, 3 * LANES), jnp.bfloat16),
            pltpu.VMEM((chunks, block // chunks, LANES), jnp.bfloat16),
            pltpu.VMEM((heads, rows, LANES), jnp.bfloat16),
            pltpu.VMEM((rows, cols), jnp.float32),
            dma((3,)),
            dma((2,)),
            dma,
            dma((owners,)),
            dma((n,)),
            dma((block // rows,)),
            dma((heads,)),
            dma,
            dma,
        ],
        compiler_params=pltpu.CompilerParams(collective_id=0, has_side_effects=True),
    )(query, key, value, q_gain.reshape(1, HD), k_gain.reshape(1, HD), out_weight)


def solution(mesh):
    blks, ulys = mesh.shape["blk"], mesh.shape["uly"]
    tokens = P(("grp", "blk", "uly"), None)
    return jax.shard_map(
        functools.partial(on_device, blks, ulys),
        mesh=mesh,
        in_specs=(tokens, tokens, tokens, P(), P(), P("uly", None)),
        out_specs=tokens,
        check_vma=False,
    )
```

```python
import functools

import jax
import jax.numpy as jnp
from jax import lax
from jax.experimental import pallas as pl
from jax.experimental.pallas import tpu as pltpu
from jax.sharding import PartitionSpec as P

HD = 96
LANES = 128
CHUNKS = 1
GROUPS = 4
MESH = pl.DeviceIdType.MESH


def loop(count, body):
    if count <= 32:
        for i in range(count):
            body(i)
    else:
        lax.fori_loop(0, count, lambda i, c: (body(i), c)[1], 0)


def take(ref, sem):
    pltpu.make_async_copy(ref, ref, sem).wait()


def layer_kernel(
    blks, ulys, heads, copies,
    q_hbm, k_hbm, v_hbm, qg_hbm, kg_hbm, w_hbm, out_ref,
    raw, gains, w_vmem, pack, qkv, attn, back, acc,
    load_sem, gain_sem, w_sem, send1, recv1, send2, recv2, send_w, recv_w,
):
    n = blks * ulys
    rows = raw.shape[1]
    owners = heads * copies
    blk, uly = lax.axis_index("blk"), lax.axis_index("uly")
    me = blk * ulys + uly
    seq = n * rows
    block = seq // copies
    chunks = CHUNKS
    chunk = block // chunks
    groups = recv2.shape[0]
    members = heads // groups
    targets = chunk // rows
    depth = w_hbm.shape[0]
    upper = (2 * me) // n

    barrier = pltpu.get_barrier_semaphore()

    def greet(i):
        d = lax.rem(me + n // 2 + i + i // (n // 2), n)
        pl.semaphore_signal(
            barrier, inc=1, device_id={"blk": d // ulys, "uly": d % ulys}, device_id_type=MESH
        )

    loop(n - 1, greet)

    loads = [
        pltpu.make_async_copy(src, raw.at[i], load_sem.at[i])
        for i, src in enumerate((q_hbm, k_hbm, v_hbm))
    ]
    load_gains = [
        pltpu.make_async_copy(src, gains.at[i], gain_sem)
        for i, src in enumerate((qg_hbm, kg_hbm))
    ]
    for one in loads + load_gains:
        one.start()

    def mirror(d):
        plane = d // 4
        return d + (plane % 2) * (3 - 2 * (d % 4))

    def owner_device(o):
        return mirror(o * n // owners)

    spot = mirror(me)
    slot = (spot * owners + n - 1) // n
    is_owner = jnp.logical_and(slot < owners, (slot * n) // owners == spot)
    slot = jnp.minimum(slot, owners - 1)

    my_depth = pl.ds(pl.multiple_of(uly * depth, depth), depth)
    load_w = pltpu.make_async_copy(w_hbm, w_vmem.at[my_depth], w_sem)
    load_w.start()

    pad = jnp.zeros((rows, LANES - HD), jnp.bfloat16)
    take(gains, gain_sem)
    for i in range(2):
        loads[i].wait()
        gain = gains[i]
        for h in range(heads):
            x = raw[i, :, h * HD:(h + 1) * HD].astype(jnp.float32)
            scale = lax.rsqrt(jnp.mean(x * x, axis=-1, keepdims=True) + 1e-06)
            normed = (x * scale * gain).astype(jnp.bfloat16)
            pack[h, :, i * LANES:(i + 1) * LANES] = jnp.concatenate([normed, pad], axis=1)
    loads[2].wait()
    for h in range(heads):
        x = raw[2, :, h * HD:(h + 1) * HD]
        pack[h, :, 2 * LANES:3 * LANES] = jnp.concatenate([x, pad], axis=1)

    pl.semaphore_wait(barrier, n - 1)

    my_rows = pl.ds(pl.multiple_of(me * rows, rows), rows)

    def send_of(o):
        d = owner_device(o)
        return d, pltpu.make_async_remote_copy(
            src_ref=pack.at[o // copies],
            dst_ref=qkv.at[my_rows],
            send_sem=send1,
            recv_sem=recv1,
            device_id={"blk": d // ulys, "uly": d % ulys},
            device_id_type=MESH,
        )

    def send(i):
        d, copy = send_of(owners - 1 - i + upper * (2 * i + 1 - owners))

        @pl.when(d != me)
        def _():
            copy.start()

    loop(owners, send)

    give_w = pltpu.make_async_remote_copy(
        src_ref=w_hbm,
        dst_ref=w_vmem.at[my_depth],
        send_sem=send_w,
        recv_sem=recv_w,
        device_id={"blk": blk, "uly": 1 - uly},
        device_id_type=MESH,
    )
    give_w.start()

    @pl.when(is_owner)
    def _():
        head = slot // copies
        part = slot % copies
        qkv[my_rows, :] = pack[head]

        take(qkv.at[pl.ds(0, (n - 1) * rows)], recv1)
        score_scale = float(HD) ** (-0.5)

        def step(query, j, carry):
            weighted, total = carry
            here = pl.ds(j * block, block)
            keys = qkv[here, LANES:2 * LANES]
            values = qkv[here, 2 * LANES:3 * LANES]
            scores = lax.dot_general(
                query, keys, (((1,), (1,)), ((), ())), preferred_element_type=jnp.float32
            ) * score_scale
            expd = jnp.exp(scores)
            total = total + jnp.sum(expd, axis=-1, keepdims=True)
            weighted = weighted + jnp.dot(
                expd.astype(jnp.bfloat16), values, preferred_element_type=jnp.float32
            )
            return weighted, total

        def result_copies(c):
            for i in range(targets):
                d = (part * chunks + c) * targets + i
                src = attn.at[pl.ds(pl.multiple_of((c * targets + i) * rows, rows), rows)]
                yield (
                    d == me,
                    functools.partial(
                        pltpu.make_async_copy, src, back.at[head], recv2.at[head // members]
                    ),
                    pltpu.make_async_remote_copy(
                        src_ref=src,
                        dst_ref=back.at[head],
                        send_sem=send2,
                        recv_sem=recv2.at[head // members],
                        device_id={"blk": d // ulys, "uly": d % ulys},
                        device_id_type=MESH,
                    ),
                )

        for k in range(chunks):
            c = chunks - 1 - k + upper * (2 * k + 1 - chunks)
            at = part * block + c * chunk
            query = qkv[pl.ds(pl.multiple_of(at, chunk), chunk), 0:LANES]
            carry = (jnp.zeros((chunk, LANES), jnp.float32), jnp.zeros((chunk, 1), jnp.float32))
            if copies == 1:
                weighted, total = step(query, 0, carry)
            else:
                weighted, total = lax.fori_loop(
                    0, copies, functools.partial(lambda q, j, c: step(q, j, c), query), carry
                )
            attn[pl.ds(pl.multiple_of(c * chunk, chunk), chunk), :] = (weighted / total).astype(jnp.bfloat16)
            for home, local, remote in result_copies(c):
                pl.when(home)(lambda local=local: local().start())
                pl.when(jnp.logical_not(home))(remote.start)

    load_w.wait()
    give_w.wait_recv()
    first = (me * groups) // n
    for i in range(groups):
        g = lax.rem(first + i * (1 - 2 * upper) + groups, groups)
        take(back.at[pl.ds(g * members, members)], recv2.at[g])
        term = jnp.dot(
            jnp.concatenate([back[g * members + j, :, 0:HD] for j in range(members)], axis=1),
            w_vmem[pl.ds(pl.multiple_of(g * members * HD, members * HD), members * HD), :],
            preferred_element_type=jnp.float32,
        )
        if i == 0:
            acc[...] = term
        elif i < groups - 1:
            acc[...] += term
        else:
            out_ref[...] = (acc[...] + term).astype(out_ref.dtype)

    give_w.wait_send()
    for i in range(copies - 1):
        take(pack, send1)

    @pl.when(is_owner)
    def _():
        take(pack.at[pl.ds(0, heads - 1)], send1)
        at_home = (slot % copies) * block == (me * rows) // block * block
        pl.when(at_home)(lambda: take(attn.at[pl.ds(0, block - rows)], send2))
        pl.when(jnp.logical_not(at_home))(lambda: take(attn, send2))

    @pl.when(jnp.logical_not(is_owner))
    def _():
        take(pack, send1)


def on_device(blks, ulys, query, key, value, q_gain, k_gain, out_weight):
    rows, width = query.shape
    heads = width // HD
    n = blks * ulys
    copies = 1
    while heads * copies * 2 <= n:
        copies *= 2
    owners = heads * copies
    depth, cols = out_weight.shape
    seq = n * rows
    block = seq // copies
    dma = pltpu.SemaphoreType.DMA
    return pl.pallas_call(
        functools.partial(layer_kernel, blks, ulys, heads, copies),
        out_shape=pltpu.VMEM((rows, cols), jnp.bfloat16),
        in_specs=[pl.BlockSpec(memory_space=pltpu.HBM)] * 6,
        out_specs=pl.BlockSpec(memory_space=pltpu.VMEM),
        scratch_shapes=[
            pltpu.VMEM((3, rows, width), jnp.bfloat16),
            pltpu.VMEM((2, 1, HD), jnp.float32),
            pltpu.VMEM((width, cols), jnp.bfloat16),
            pltpu.VMEM((heads, rows, 3 * LANES), jnp.bfloat16),
            pltpu.VMEM((seq, 3 * LANES), jnp.bfloat16),
            pltpu.VMEM((block, LANES), jnp.bfloat16),
            pltpu.VMEM((heads, rows, LANES), jnp.bfloat16),
            pltpu.VMEM((rows, cols), jnp.float32),
            dma((3,)),
            dma,
            dma,
            dma,
            dma,
            dma,
            dma((GROUPS,)),
            dma,
            dma,
        ],
        compiler_params=pltpu.CompilerParams(collective_id=0, has_side_effects=True),
    )(query, key, value, q_gain.reshape(1, HD), k_gain.reshape(1, HD), out_weight)


def solution(mesh):
    blks, ulys = mesh.shape["blk"], mesh.shape["uly"]
    tokens = P(("grp", "blk", "uly"), None)
    return jax.shard_map(
        functools.partial(on_device, blks, ulys),
        mesh=mesh,
        in_specs=(tokens, tokens, tokens, P(), P(), P("uly", None)),
        out_specs=tokens,
        check_vma=False,
    )
```

```python
import functools

import jax
import jax.numpy as jnp
from jax import lax
from jax.experimental import pallas as pl
from jax.experimental.pallas import tpu as pltpu
from jax.sharding import PartitionSpec as P

HD = 96
LANES = 128
CHUNKS = 1
GROUPS = 4
MESH = pl.DeviceIdType.MESH


def loop(count, body):
    if count <= 32:
        for i in range(count):
            body(i)
    else:
        lax.fori_loop(0, count, lambda i, c: (body(i), c)[1], 0)


def take(ref, sem):
    pltpu.make_async_copy(ref, ref, sem).wait()


def layer_kernel(
    blks, ulys, heads, copies,
    q_hbm, k_hbm, v_hbm, qg_hbm, kg_hbm, w_hbm, out_ref,
    raw, gains, w_vmem, pack, qkv, attn, back, acc,
    load_sem, gain_sem, w_sem, send1, recv1, send2, recv2, send_w, recv_w,
):
    n = blks * ulys
    rows = raw.shape[1]
    owners = heads * copies
    blk, uly = lax.axis_index("blk"), lax.axis_index("uly")
    me = blk * ulys + uly
    seq = n * rows
    block = seq // copies
    chunks = CHUNKS
    chunk = block // chunks
    groups = recv2.shape[0]
    members = heads // groups
    targets = chunk // rows
    depth = w_hbm.shape[0]
    upper = (2 * me) // n

    barrier = pltpu.get_barrier_semaphore()

    def greet(i):
        d = lax.rem(me + n // 2 + i + i // (n // 2), n)
        pl.semaphore_signal(
            barrier, inc=1, device_id={"blk": d // ulys, "uly": d % ulys}, device_id_type=MESH
        )

    loop(n - 1, greet)

    loads = [
        pltpu.make_async_copy(src, raw.at[i], load_sem.at[i])
        for i, src in enumerate((q_hbm, k_hbm, v_hbm))
    ]
    load_gains = [
        pltpu.make_async_copy(src, gains.at[i], gain_sem)
        for i, src in enumerate((qg_hbm, kg_hbm))
    ]
    for one in loads + load_gains:
        one.start()

    def mirror(d):
        plane = d // 4
        return d + (plane % 2) * (3 - 2 * (d % 4))

    def owner_device(o):
        return mirror(o * n // owners)

    spot = mirror(me)
    slot = (spot * owners + n - 1) // n
    is_owner = jnp.logical_and(slot < owners, (slot * n) // owners == spot)
    slot = jnp.minimum(slot, owners - 1)

    my_depth = pl.ds(pl.multiple_of(uly * depth, depth), depth)
    load_w = pltpu.make_async_copy(w_hbm, w_vmem.at[my_depth], w_sem)
    load_w.start()

    pad = jnp.zeros((rows, LANES - HD), jnp.bfloat16)
    take(gains, gain_sem)
    for i in range(2):
        loads[i].wait()
        gain = gains[i]
        for h in range(heads):
            x = raw[i, :, h * HD:(h + 1) * HD].astype(jnp.float32)
            scale = lax.rsqrt(jnp.mean(x * x, axis=-1, keepdims=True) + 1e-06)
            normed = (x * scale * gain).astype(jnp.bfloat16)
            pack[h, :, i * LANES:(i + 1) * LANES] = jnp.concatenate([normed, pad], axis=1)
    loads[2].wait()
    for h in range(heads):
        x = raw[2, :, h * HD:(h + 1) * HD]
        pack[h, :, 2 * LANES:3 * LANES] = jnp.concatenate([x, pad], axis=1)

    pl.semaphore_wait(barrier, n - 1)

    my_rows = pl.ds(pl.multiple_of(me * rows, rows), rows)

    def send_of(o):
        d = owner_device(o)
        return d, pltpu.make_async_remote_copy(
            src_ref=pack.at[o // copies],
            dst_ref=qkv.at[my_rows],
            send_sem=send1,
            recv_sem=recv1,
            device_id={"blk": d // ulys, "uly": d % ulys},
            device_id_type=MESH,
        )

    def send(i):
        d, copy = send_of(owners - 1 - i + upper * (2 * i + 1 - owners))

        @pl.when(d != me)
        def _():
            copy.start()

    loop(owners, send)

    give_w = pltpu.make_async_remote_copy(
        src_ref=w_hbm,
        dst_ref=w_vmem.at[my_depth],
        send_sem=send_w,
        recv_sem=recv_w,
        device_id={"blk": blk, "uly": 1 - uly},
        device_id_type=MESH,
    )
    give_w.start()

    @pl.when(is_owner)
    def _():
        head = slot // copies
        part = slot % copies
        qkv[my_rows, :] = pack[head]

        take(qkv.at[pl.ds(0, (n - 1) * rows)], recv1)
        score_scale = float(HD) ** (-0.5)

        def step(query, j, carry):
            weighted, total = carry
            here = pl.ds(j * block, block)
            keys = qkv[here, LANES:2 * LANES]
            values = qkv[here, 2 * LANES:3 * LANES]
            scores = lax.dot_general(
                query, keys, (((1,), (1,)), ((), ())), preferred_element_type=jnp.float32
            ) * score_scale
            expd = jnp.exp(scores)
            total = total + jnp.sum(expd, axis=-1, keepdims=True)
            weighted = weighted + jnp.dot(
                expd.astype(jnp.bfloat16), values, preferred_element_type=jnp.float32
            )
            return weighted, total

        def result_copies(c):
            for k in range(targets):
                i = targets - 1 - k + upper * (2 * k + 1 - targets)
                d = (part * chunks + c) * targets + i
                src = attn.at[pl.ds(pl.multiple_of((c * targets + i) * rows, rows), rows)]
                yield (
                    d == me,
                    functools.partial(
                        pltpu.make_async_copy, src, back.at[head], recv2.at[head // members]
                    ),
                    pltpu.make_async_remote_copy(
                        src_ref=src,
                        dst_ref=back.at[head],
                        send_sem=send2,
                        recv_sem=recv2.at[head // members],
                        device_id={"blk": d // ulys, "uly": d % ulys},
                        device_id_type=MESH,
                    ),
                )

        for k in range(chunks):
            c = chunks - 1 - k + upper * (2 * k + 1 - chunks)
            at = part * block + c * chunk
            query = qkv[pl.ds(pl.multiple_of(at, chunk), chunk), 0:LANES]
            carry = (jnp.zeros((chunk, LANES), jnp.float32), jnp.zeros((chunk, 1), jnp.float32))
            if copies == 1:
                weighted, total = step(query, 0, carry)
            else:
                weighted, total = lax.fori_loop(
                    0, copies, functools.partial(lambda q, j, c: step(q, j, c), query), carry
                )
            attn[pl.ds(pl.multiple_of(c * chunk, chunk), chunk), :] = (weighted / total).astype(jnp.bfloat16)
            for home, local, remote in result_copies(c):
                pl.when(home)(lambda local=local: local().start())
                pl.when(jnp.logical_not(home))(remote.start)

    load_w.wait()
    give_w.wait_recv()
    first = (me * groups) // n
    for i in range(groups):
        g = lax.rem(first + i * (1 - 2 * upper) + groups, groups)
        take(back.at[pl.ds(g * members, members)], recv2.at[g])
        for j in range(members):
            h = g * members + j
            term = jnp.dot(
                back[h, :, 0:HD],
                w_vmem[pl.ds(pl.multiple_of(h * HD, HD), HD), :],
                preferred_element_type=jnp.float32,
            )
            if i == 0 and j == 0:
                acc[...] = term
            elif i < groups - 1 or j < members - 1:
                acc[...] += term
            else:
                out_ref[...] = (acc[...] + term).astype(out_ref.dtype)

    give_w.wait_send()
    for i in range(copies - 1):
        take(pack, send1)

    @pl.when(is_owner)
    def _():
        take(pack.at[pl.ds(0, heads - 1)], send1)
        at_home = (slot % copies) * block == (me * rows) // block * block
        pl.when(at_home)(lambda: take(attn.at[pl.ds(0, block - rows)], send2))
        pl.when(jnp.logical_not(at_home))(lambda: take(attn, send2))

    @pl.when(jnp.logical_not(is_owner))
    def _():
        take(pack, send1)


def on_device(blks, ulys, query, key, value, q_gain, k_gain, out_weight):
    rows, width = query.shape
    heads = width // HD
    n = blks * ulys
    copies = 1
    while heads * copies * 2 <= n:
        copies *= 2
    owners = heads * copies
    depth, cols = out_weight.shape
    seq = n * rows
    block = seq // copies
    dma = pltpu.SemaphoreType.DMA
    return pl.pallas_call(
        functools.partial(layer_kernel, blks, ulys, heads, copies),
        out_shape=pltpu.VMEM((rows, cols), jnp.bfloat16),
        in_specs=[pl.BlockSpec(memory_space=pltpu.HBM)] * 6,
        out_specs=pl.BlockSpec(memory_space=pltpu.VMEM),
        scratch_shapes=[
            pltpu.VMEM((3, rows, width), jnp.bfloat16),
            pltpu.VMEM((2, 1, HD), jnp.float32),
            pltpu.VMEM((width, cols), jnp.bfloat16),
            pltpu.VMEM((heads, rows, 3 * LANES), jnp.bfloat16),
            pltpu.VMEM((seq, 3 * LANES), jnp.bfloat16),
            pltpu.VMEM((block, LANES), jnp.bfloat16),
            pltpu.VMEM((heads, rows, LANES), jnp.bfloat16),
            pltpu.VMEM((rows, cols), jnp.float32),
            dma((3,)),
            dma,
            dma,
            dma,
            dma,
            dma,
            dma((GROUPS,)),
            dma,
            dma,
        ],
        compiler_params=pltpu.CompilerParams(collective_id=0, has_side_effects=True),
    )(query, key, value, q_gain.reshape(1, HD), k_gain.reshape(1, HD), out_weight)


def solution(mesh):
    blks, ulys = mesh.shape["blk"], mesh.shape["uly"]
    tokens = P(("grp", "blk", "uly"), None)
    return jax.shard_map(
        functools.partial(on_device, blks, ulys),
        mesh=mesh,
        in_specs=(tokens, tokens, tokens, P(), P(), P("uly", None)),
        out_specs=tokens,
        check_vma=False,
    )
```
